32 devices in a mesh: freq: 8 (over y, x, core), base: 4 (over z).
Axes of the slice: x: 2, y: 2, z: 4, core: 2. Of those that a mesh axis runs over, the one named last changes fastest.
Arguments:
- visibility: float32 [2, 16, 2048], P(None, 'freq', 'base'), may hold values from -6 to 6
- tile_of: int32 [16, 2048, 1], P('freq', 'base'), may hold values from 0 to 3; in each aligned block of 512 rows (0 to 511, 512 to 1023, ..., all dimensions but the last counted through in order) at most 256 rows name the same one
- u_within: int32 [16, 2048], P('freq', 'base'), may hold values from 0 to 255
- v_cell: int32 [16, 2048], P('freq', 'base'), may hold values from 0 to 1016
- kernel_index: int32 [2, 16, 2048], P(None, 'freq', 'base'), may hold values from 0 to 127
- kernel: float32 [128, 8], replicated, may hold values from 0.1 to 1
- live_count: int32 [16, 4], P('freq', 'base'), may hold values from 64 to 512, as said below
- bin_map: int32 [1024, 1024], P('base'), may hold values from 0 to 511, as said below
Outputs:
- power_map: float32 [1024, 1024], P('freq', 'base')
- spectrum: float32 [512], replicated
The draws below stay inside these ranges and needn't reach their ends.
Inputs may be any that keep to these rules, and one draw needn't show every extreme that they name: `tile_of`: among the visibilities of one channel on one device, at most 256 name the same tile, and in some device's visibilities a tile is named by exactly 256. `live_count`: the first device along base holds 512 used slots in every channel; the used slots of a device are its first ones. `bin_map`: every bin number occurs.
All inputs are finite; a program needn't handle non-finite values.
Results may differ from the reference program's by a relative error of at most 0.0003.
Values sent between devices are 32-bit elements; how exact they have to be, the bound alone decides.
No kernel may reach another device: no remote copies, remote signals or barrier semaphores. Data moves between devices by JAX's collectives and lax.ppermute only.
A program may use at most 128 MiB of HBM per device.

```python
import math
import jax
import jax.numpy as jnp
import numpy as np
from jax import lax

G = 1024
NBINS = 512
KW = 8
OVER = 128
VIS_DEV = 512
CH_DEV = 2
TILE = 256
CAP = 256
CH = 16
VIS = 2048
N_FREQ = 8
N_BASE = 4


def draw_visibility(key, part):
    channels = CH_DEV * N_FREQ
    visits = VIS_DEV * N_BASE
    frequency = 100.0 + 60.0 * jnp.arange(channels, dtype=jnp.float32) / max(channels - 1, 1)
    falloff = (frequency / 100.0) ** (-2.6)
    values = jnp.clip(jax.random.normal(key, (2, channels, visits), jnp.float32), -6.0, 6.0)
    return values * falloff[None, :, None]


def draw_live_count(key, part):
    channels = CH_DEV * N_FREQ
    floor_count = VIS_DEV // 8
    device = jnp.arange(N_BASE, dtype=jnp.int32)
    spread = (VIS_DEV - floor_count) * (N_BASE - device) // N_BASE + 1
    additional = jax.random.randint(key, (channels, N_BASE), 0, spread[None, :])
    counts = floor_count + additional
    return jnp.where(device[None, :] == 0, VIS_DEV, counts).astype(jnp.int32)


def draw_bin_map(key, part):
    centre = jax.random.randint(key, (2,), -(G // 8), G // 8 + 1)
    positions = jnp.arange(G, dtype=jnp.int32)
    along_u = (positions - centre[0] + G // 2) % G - G // 2
    along_v = (positions - centre[1] + G // 2) % G - G // 2
    radius_sq = along_u[:, None] * along_u[:, None] + along_v[None, :] * along_v[None, :]
    return jnp.minimum(radius_sq * NBINS // (G // 2 * (G // 2)), NBINS - 1).astype(jnp.int32)


def plant(entries, stream_key, low, high):
    extent = entries.shape
    spot = [jax.random.randint(jax.random.fold_in(stream_key, axis), (), 0, extent[axis]) for axis in range(len(extent))]
    entries = entries.at[tuple(spot)].set(low)
    longest = extent.index(max(extent))
    spot[longest] = (spot[longest] + 1) % extent[longest]
    return entries.at[tuple(spot)].set(high)


def deal_out(key, own, number, rows, number_of, top, bound, slope):
    order = jax.random.permutation(key, number_of)
    heavy_load, usual = shares(number_of, rows * top, bound, slope, True), shares(number_of, rows * top, bound, slope, False)
    places = jnp.arange(number_of)

    def named(tallies, rotation):
        used = int((tallies > 0).sum())
        fixed = max(1, used // 4)
        passed = fixed + (places - fixed + rotation * (used - fixed)) % max(1, number_of - fixed)
        return jnp.zeros((number_of,), jnp.int32).at[order[jnp.where(places < fixed, places, passed)]].set(jnp.asarray(tallies, jnp.int32))

    tallies = jnp.where(number % 4 == 0, named(heavy_load, number // 4), named(usual, number - number // 4 - 1))
    mixed = jax.random.permutation(jax.random.fold_in(own, 3), number_of)
    giver, receiver = mixed[0:number_of // 2 * 2:2], mixed[1:number_of // 2 * 2:2]
    margin = jnp.minimum(tallies[giver] - 1, bound - tallies[receiver]) // 2
    margin = jnp.where((giver == order[0]) | (receiver == order[0]) | (tallies[receiver] == 0), 0, jnp.maximum(margin, 0))
    passed = jax.random.randint(jax.random.fold_in(own, 4), (number_of // 2,), 0, 1 << 20) % (margin + 1)
    tallies = tallies.at[giver].add(-passed).at[receiver].add(passed)
    items = jnp.searchsorted(jnp.cumsum(tallies), jnp.arange(rows * top), side="right").astype(jnp.int32)
    table = items.reshape(top, rows).T
    table = table[jax.random.permutation(jax.random.fold_in(own, 1), rows)]
    rotation = jax.random.randint(jax.random.fold_in(own, 2), (rows, 1), 0, top)
    return jnp.take_along_axis(table, (jnp.arange(top)[None, :] + rotation) % top, axis=1)


def shares(count, total, limit, skew, full):
    loads = [(1 << 20) // math.isqrt(rank ** skew) + 1 for rank in range(1, count + 1)]
    largest = limit if full else min(limit, max(-(-total // count), total * loads[0] // sum(loads)))
    least = 1 if total - largest >= count - 1 else 0
    given, surplus = [largest] + [least] * (count - 1), total - largest - least * (count - 1)
    while surplus > 0:
        free = [i for i in range(1, count) if given[i] < largest] or [i for i in range(1, count) if given[i] < limit]
        pool, remaining = sum([loads[i] for i in free]), surplus
        for i in free:
            more = min(limit - given[i], max(1, remaining * loads[i] // pool), surplus)
            given[i] = given[i] + more
            surplus = surplus - more
    return np.array(given)


def setup_inputs(seed: int = 0) -> dict:
    key_list = jax.random.split(jax.random.key(seed), 9)
    visibility = draw_visibility(jax.random.fold_in(key_list[8], 71), 0)
    tile_of_keys = jax.random.split(jax.random.fold_in(key_list[1], 1), CH * VIS // VIS_DEV)
    tile_of_turns = jax.random.permutation(jax.random.fold_in(key_list[1], 3), CH * VIS // VIS_DEV)
    tile_of = jax.vmap(lambda own, number: deal_out(jax.random.fold_in(key_list[1], 2), own, number, VIS_DEV, N_BASE, 1, CAP, 2))(tile_of_keys, tile_of_turns).reshape((CH, VIS, 1))
    u_within = plant(jax.random.randint(key_list[2], (CH, VIS), 0, TILE), jax.random.fold_in(key_list[2], 1), 0, TILE - 1).astype(jnp.int32)
    v_cell = plant(jax.random.randint(key_list[3], (CH, VIS), 0, G - KW + 1), jax.random.fold_in(key_list[3], 1), 0, G - KW).astype(jnp.int32)
    kernel_index = plant(jax.random.randint(key_list[4], (2, CH, VIS), 0, OVER), jax.random.fold_in(key_list[4], 1), 0, OVER - 1).astype(jnp.int32)
    kernel = jnp.clip(jnp.exp(jax.random.uniform(key_list[5], (OVER, KW), jnp.float32, math.log(0.1), math.log(1.0))), 0.1, 1.0)
    live_count = draw_live_count(jax.random.fold_in(key_list[8], 71), 0)
    bin_map = draw_bin_map(jax.random.fold_in(key_list[8], 71), 0)
    return {"visibility": visibility, "tile_of": tile_of, "u_within": u_within, "v_cell": v_cell, "kernel_index": kernel_index, "kernel": kernel, "live_count": live_count, "bin_map": bin_map}


def channel_power(visibility_re, visibility_im, tile_row, u_within, v_cell, index_u, index_v, used_slots, kernel):
    tile_rows = G // N_BASE
    u_cell = jnp.minimum(tile_row * tile_rows + u_within, G - KW)
    position = jnp.arange(VIS_DEV * N_BASE, dtype=jnp.int32)
    holder = position // VIS_DEV
    is_live = (position % VIS_DEV) < used_slots[holder]
    zeroed = jnp.zeros_like(visibility_re)
    real_part = jnp.where(is_live, visibility_re, zeroed)
    imag_part = jnp.where(is_live, visibility_im, zeroed)
    taps_u = kernel[index_u]
    taps_v = kernel[index_v]
    weight = taps_u[:, :, None] * taps_v[:, None, :]
    offsets = jnp.arange(KW, dtype=jnp.int32)
    row_cells = jnp.broadcast_to(u_cell[:, None, None] + offsets[None, :, None], weight.shape)
    col_cells = jnp.broadcast_to(v_cell[:, None, None] + offsets[None, None, :], weight.shape)
    grid_re = jnp.zeros((G, G), jnp.float32).at[row_cells, col_cells].add(weight * real_part[:, None, None])
    grid_im = jnp.zeros((G, G), jnp.float32).at[row_cells, col_cells].add(weight * imag_part[:, None, None])
    transformed = jnp.fft.fft2(grid_re + 1j * grid_im)
    return transformed.real * transformed.real + transformed.imag * transformed.imag


def reference(visibility, tile_of, u_within, v_cell, kernel_index, kernel, live_count, bin_map):
    def accumulate(running, channel_items):
        vis_re, vis_im, tile_row, within, column, index_u, index_v, used_slots = channel_items
        return running + channel_power(vis_re, vis_im, tile_row, within, column, index_u, index_v, used_slots, kernel), None

    channel_items = (visibility[0], visibility[1], tile_of[:, :, 0], u_within, v_cell, kernel_index[0], kernel_index[1], live_count)
    power_sum, _ = lax.scan(accumulate, jnp.zeros((G, G), jnp.float32), channel_items)
    channels = CH_DEV * N_FREQ
    visits = VIS_DEV * N_BASE
    power_map = power_sum / (channels * visits)
    flat_bins = bin_map.T.reshape(-1)
    totals = jax.ops.segment_sum(power_map.reshape(-1), flat_bins, num_segments=NBINS)
    counts = jax.ops.segment_sum(jnp.ones_like(power_map).reshape(-1), flat_bins, num_segments=NBINS)
    return power_map, totals / counts
```

```python
import functools

import jax
import jax.numpy as jnp
import numpy as np
from jax import lax
from jax.experimental import pallas as pl
from jax.experimental.pallas import tpu as pltpu
from jax.sharding import PartitionSpec as P

G = 1024
NBINS = 512
KW = 8
RADIX = 4
SUB = G // RADIX
CHUNK = 256
LANES = 128
V_LOW = 32
V_HIGH = G // V_LOW
BIN_LOW = 16
BIN_HIGH = NBINS // BIN_LOW
F32 = jnp.float32
BF16 = jnp.bfloat16


def np_split(x):
    high = x.astype(np.float32).astype(jnp.bfloat16)
    low = (x - high.astype(np.float64)).astype(np.float32).astype(jnp.bfloat16)
    return high, low


def split(x):
    high = x.astype(BF16)
    return high, (x - high.astype(F32)).astype(BF16)


def row_dft_tables():
    k = np.arange(SUB)[:, None]
    tables = []
    for first in range(RADIX):
        u = RADIX * np.arange(SUB)[None, :] + first
        angle = 2 * np.pi * (k * u % G) / G
        high, low = np_split(np.concatenate([np.cos(angle), np.sin(angle)], 0))
        tables.append(np.concatenate([high, low], 1))
    return np.stack(tables)


def phases(cells, peers):
    columns = np.arange(G)[:, None]
    angle = 2 * np.pi * (columns * cells[None, :] % G) / G
    width = G // peers
    shape = (peers, width, len(cells))
    return np.cos(angle).reshape(shape), np.sin(angle).reshape(shape)


def column_tables(peers):
    cosine, sine = phases(V_LOW * np.arange(V_HIGH), peers)
    coarse = np.concatenate(
        [np.concatenate([cosine, sine], 2), np.concatenate([-sine, cosine], 2)], 1
    )
    high, low = np_split(coarse)
    coarse = np.concatenate([high, low, high], 2)
    cosine, sine = phases(np.arange(V_LOW), peers)
    high, low = np_split(np.concatenate([cosine, -sine], 1))
    fine = np.concatenate([high, low], 2)
    cosine, sine = phases(np.arange(KW), peers)
    taps = np.concatenate([cosine, -sine], 1).astype(np.float32)
    return coarse, fine, taps


def dot(a, b, transposed=False, **kw):
    dims = (((1,), (1,)), ((), ())) if transposed else (((1,), (0,)), ((), ()))
    return lax.dot_general(a, b, dims, preferred_element_type=F32, **kw)


def image_kernel(
    base_ref, live_ref, gathered_ref, kernel_ref, row_ref, coarse_ref, fine_ref, tap_ref,
    out_ref, packed_ref, spectrum_ref, kernel_halves_ref, grid_ref, *, normalizer,
):
    channel = pl.program_id(0)
    peers, _, _, slots = gathered_ref.shape
    width = out_ref.shape[1]
    table_rows = kernel_ref.shape[1]

    @pl.when(channel == 0)
    def _():
        high, low = split(
            dot(tap_ref[...], kernel_ref[...], precision=lax.Precision.HIGHEST)
        )
        spectrum_ref[...] = jnp.concatenate([high, low], axis=1)
        high = kernel_ref[...].astype(BF16).astype(F32)
        kernel_halves_ref[...] = jnp.concatenate([high, kernel_ref[...] - high], axis=0)

    packed_ref[...] = jnp.zeros_like(packed_ref)
    offset = jnp.int32(0)
    lane = lax.broadcasted_iota(jnp.int32, (8, slots + LANES), 1)
    for peer in range(peers):
        live = live_ref[peer, channel]
        block = offset // LANES
        within = offset - block * LANES
        fields = jnp.concatenate(
            [gathered_ref[peer, 0], jnp.zeros((8, LANES), F32)], axis=1
        )
        fields = pltpu.roll(fields, within, 1)
        kept = (lane >= within) & (lane < within + live)
        window = pl.ds(pl.multiple_of(block * LANES, LANES), slots + LANES)
        packed_ref[:, window] = packed_ref[:, window] + jnp.where(kept, fields, 0.0)
        offset = offset + live

    grid_ref[...] = jnp.zeros_like(grid_ref)

    def add_chunk(index, carry):
        fields = packed_ref[:, pl.ds(pl.multiple_of(index * CHUNK, CHUNK), CHUNK)]
        real, imag = fields[0:1], fields[1:2]
        cells = fields[2:6].astype(jnp.int32)
        u_cell, v_cell, index_u, index_v = cells[0:1], cells[1:2], cells[2:3], cells[3:4]
        table_row = lax.broadcasted_iota(jnp.int32, (table_rows, CHUNK), 0)
        chosen_v = jnp.where(table_row == index_v, 1.0, 0.0).astype(BF16)
        footprint = dot(spectrum_ref[...], jnp.concatenate([chosen_v, chosen_v], axis=0))
        high_row = lax.broadcasted_iota(jnp.int32, (V_HIGH, CHUNK), 0)
        at_coarse = high_row == v_cell // V_LOW
        values = jnp.concatenate(
            [jnp.where(at_coarse, real, 0.0), jnp.where(at_coarse, imag, 0.0)], axis=0
        )
        high, low = split(values)
        coarse = dot(coarse_ref[...], jnp.concatenate([high, high, low], axis=0))
        low_row = lax.broadcasted_iota(jnp.int32, (V_LOW, CHUNK), 0)
        at_fine = jnp.where(low_row == v_cell % V_LOW, 1.0, 0.0).astype(BF16)
        fine = dot(fine_ref[...], jnp.concatenate([at_fine, at_fine], axis=0))
        a_re, a_im = coarse[:width], coarse[width:]
        b_re, b_im = fine[:width], fine[width:]
        c_re = a_re * b_re - a_im * b_im
        c_im = a_re * b_im + a_im * b_re
        d_re, d_im = footprint[:width], footprint[width:]
        column = jnp.concatenate(
            [c_re * d_re - c_im * d_im, c_re * d_im + c_im * d_re], axis=0
        )
        high, low = split(column)
        column = jnp.concatenate([high, low, high], axis=1)

        chosen_u = jnp.where(table_row == index_u, 1.0, 0.0).astype(BF16)
        taps = dot(kernel_halves_ref[...].astype(BF16), chosen_u)
        grid_row = lax.broadcasted_iota(jnp.int32, (SUB, CHUNK), 0)
        rows = []
        for first in range(RADIX):
            tap = (first - u_cell) & (RADIX - 1)
            start = (u_cell + tap - first) // RADIX

            def tap_of(base):
                value = taps[base : base + 1]
                for t in range(1, RADIX):
                    value = jnp.where(tap == t, taps[base + t : base + t + 1], value)
                return value

            at_first = grid_row == start
            at_second = grid_row == start + 1
            halves = []
            for base in (0, KW):
                part = jnp.where(
                    at_first, tap_of(base), jnp.where(at_second, tap_of(base + RADIX), 0.0)
                )
                halves.append(part.astype(BF16))
            rows.append(jnp.concatenate([halves[0], halves[0], halves[1]], axis=1))
        grid_ref[...] += dot(jnp.concatenate(rows, axis=0), column, transposed=True)
        return carry

    lax.fori_loop(0, (offset + CHUNK - 1) // CHUNK, add_chunk, 0)

    parts = []
    for first in range(RADIX):
        high, low = split(grid_ref[first * SUB : (first + 1) * SUB, :])
        table = row_ref[first]
        table = jnp.concatenate([table[:, :SUB], table], axis=1)
        both = dot(table, jnp.concatenate([high, low, high], axis=0))
        re = both[:SUB, :width] + both[SUB:, width:]
        im = both[:SUB, width:] - both[SUB:, :width]
        parts.append((re, im))
    (r0, i0), (r1, i1), (r2, i2), (r3, i3) = parts
    ar, ai, br, bi = r0 + r2, i0 + i2, r0 - r2, i0 - i2
    cr, ci, dr, di = r1 + r3, i1 + i3, r1 - r3, i1 - i3
    images = [
        (ar + cr, ai + ci),
        (br + di, bi - dr),
        (ar - cr, ai - ci),
        (br - di, bi + dr),
    ]
    for block, (re, im) in enumerate(images):
        window = slice(block * SUB, (block + 1) * SUB)
        power = (re * re + im * im) * normalizer

        @pl.when(channel == 0)
        def _():
            out_ref[window, :] = power

        @pl.when(channel != 0)
        def _():
            out_ref[window, :] += power


def image_power(base_index, live, gathered, kernel, normalizer):
    peers, channels, _, slots = gathered.shape
    width = G // peers
    coarse, fine, taps = column_tables(peers)
    table_rows = kernel.shape[0]
    whole = lambda shape: pl.BlockSpec(shape, lambda c, *_: (0,) * len(shape))
    own = lambda x: pl.BlockSpec((None,) + x.shape[1:], lambda c, b, *_: (b[0], 0, 0))
    rows = row_dft_tables()
    spec = pltpu.PrefetchScalarGridSpec(
        num_scalar_prefetch=2,
        grid=(channels,),
        in_specs=[
            pl.BlockSpec((peers, 1, 8, slots), lambda c, *_: (0, c, 0, 0)),
            whole((KW, table_rows)),
            whole(rows.shape),
            own(coarse),
            own(fine),
            own(taps),
        ],
        out_specs=whole((G, width)),
        scratch_shapes=[
            pltpu.VMEM((8, peers * slots + LANES), F32),
            pltpu.VMEM((2 * width, 2 * table_rows), BF16),
            pltpu.VMEM((2 * KW, table_rows), F32),
            pltpu.VMEM((G, 2 * width), F32),
        ],
    )
    return pl.pallas_call(
        functools.partial(image_kernel, normalizer=normalizer),
        grid_spec=spec,
        out_shape=jax.ShapeDtypeStruct((G, width), F32),
        compiler_params=pltpu.CompilerParams(dimension_semantics=("arbitrary",)),
        name="image_power",
    )(base_index, live, gathered, kernel.T, rows, coarse, fine, taps)


def bin_kernel(freq_ref, power_ref, bins_ref, share_ref, sums_ref, bins_t_ref):
    share = power_ref[0]
    for peer in range(1, power_ref.shape[0]):
        share = share + power_ref[peer]
    share_ref[...] = share
    bins_t_ref[...] = bins_ref[...].astype(F32).T
    rows, width = share.shape
    group = 8
    high_row = lax.broadcasted_iota(jnp.int32, (BIN_HIGH, width), 0)
    low_row = lax.broadcasted_iota(jnp.int32, (BIN_LOW, width), 0)

    def add_group(index, running):
        window = pl.ds(pl.multiple_of(index * group, group), group)
        bins = bins_t_ref[window, :].astype(jnp.int32)
        values = share_ref[window, :]
        high = values.astype(BF16).astype(F32)
        rest = values - high
        middle = rest.astype(BF16).astype(F32)
        low = rest - middle
        left, right = [], []
        for row in range(group):
            one = slice(row, row + 1)
            at_high = high_row == bins[one] // BIN_LOW
            at_low = low_row == bins[one] % BIN_LOW
            left.append(jnp.where(at_high, 1.0, 0.0).astype(BF16))
            pieces = [jnp.where(at_low, x[one], 0.0) for x in (high, middle, low)]
            pieces.append(jnp.where(at_low, 1.0, 0.0))
            right.append(jnp.concatenate(pieces, axis=0).astype(BF16))
        if width % LANES == 0:
            left, right = [jnp.concatenate(left, axis=1)], [jnp.concatenate(right, axis=1)]
        for a, b in zip(left, right):
            running = running + dot(a, b, transposed=True)
        return running

    zeros = jnp.zeros((BIN_HIGH, 4 * BIN_LOW), F32)
    sums_ref[...] = lax.fori_loop(0, rows // group, add_group, zeros)


def bin_power(freq_index, received, bin_map):
    peers, rows, width = received.shape
    if rows % LANES:
        bin_map = lax.dynamic_slice_in_dim(bin_map, freq_index[0] * rows, rows, 1)
        freq_index = jnp.zeros_like(freq_index)
    spec = pltpu.PrefetchScalarGridSpec(
        num_scalar_prefetch=1,
        grid=(1,),
        in_specs=[
            pl.BlockSpec((peers, rows, width), lambda i, f: (0, 0, 0)),
            pl.BlockSpec((width, rows), lambda i, f: (0, f[0])),
        ],
        out_specs=[
            pl.BlockSpec((rows, width), lambda i, f: (0, 0)),
            pl.BlockSpec((BIN_HIGH, 4 * BIN_LOW), lambda i, f: (0, 0)),
        ],
        scratch_shapes=[pltpu.VMEM((rows, width), F32)],
    )
    return pl.pallas_call(
        bin_kernel,
        grid_spec=spec,
        out_shape=[
            jax.ShapeDtypeStruct((rows, width), F32),
            jax.ShapeDtypeStruct((BIN_HIGH, 4 * BIN_LOW), F32),
        ],
        name="bin_power",
    )(freq_index, received, bin_map)


def sent_to_all(x, axis):
    copies = jnp.broadcast_to(x[None], (lax.axis_size(axis),) + x.shape)
    return lax.all_to_all(copies, axis, split_axis=0, concat_axis=0)


def per_device(visibility, tile_of, u_within, v_cell, kernel_index, kernel, live_count, bin_map):
    base_count = lax.axis_size("base")
    freq_count = lax.axis_size("freq")
    tile_rows = G // base_count
    channels_here, slots = visibility.shape[1:]
    u_cell = jnp.minimum(tile_of[:, :, 0] * tile_rows + u_within, G - KW)
    cells = jnp.stack([u_cell, v_cell, kernel_index[0], kernel_index[1]]).astype(F32)
    counts = jnp.broadcast_to(live_count.astype(F32)[None], (1, channels_here, slots))
    fields = jnp.concatenate([visibility, cells, counts, jnp.zeros_like(counts)], axis=0)
    gathered = sent_to_all(fields.transpose(1, 0, 2), "base")
    live = gathered[:, :, 6, 0].astype(jnp.int32)
    normalizer = 1.0 / (channels_here * freq_count * slots * base_count)
    power_part = image_power(
        lax.axis_index("base")[None], live, gathered, kernel, normalizer
    )
    blocks = power_part.reshape(freq_count, G // freq_count, -1)
    received = lax.all_to_all(blocks, "freq", split_axis=0, concat_axis=0)
    power_share, sums = bin_power(lax.axis_index("freq")[None], received, bin_map)
    sums = sums.reshape(BIN_HIGH, 4, BIN_LOW)
    sums = jnp.stack([sums[:, 0] + sums[:, 1] + sums[:, 2], sums[:, 3]]).reshape(2 * NBINS)
    sums = jnp.sum(sent_to_all(sums, ("freq", "base")), axis=0)
    return power_share, sums[:NBINS] / sums[NBINS:]


def solution(mesh):
    in_specs = (
        P(None, "freq", "base"),
        P("freq", "base", None),
        P("freq", "base"),
        P("freq", "base"),
        P(None, "freq", "base"),
        P(),
        P("freq", "base"),
        P("base", None),
    )
    out_specs = (P("freq", "base"), P())
    return jax.shard_map(
        per_device, mesh=mesh, in_specs=in_specs, out_specs=out_specs, check_vma=False
    )
```

```python
import functools

import jax
import jax.numpy as jnp
import numpy as np
from jax import lax
from jax.experimental import pallas as pl
from jax.experimental.pallas import tpu as pltpu
from jax.sharding import PartitionSpec as P

G = 1024
NBINS = 512
KW = 8
RADIX = 4
TILES = 4
WINDOW = 72
BLOCK = 264
SUB = G // RADIX
CHUNK = 256
LANES = 128
V_LOW = 32
V_HIGH = G // V_LOW
BIN_LOW = 128
BIN_HIGH = NBINS // BIN_LOW
F32 = jnp.float32
BF16 = jnp.bfloat16


def np_split(x):
    high = x.astype(np.float32).astype(jnp.bfloat16)
    low = (x - high.astype(np.float64)).astype(np.float32).astype(jnp.bfloat16)
    return high, low


def split(x):
    high = x.astype(BF16)
    return high, (x - high.astype(F32)).astype(BF16)


def row_dft_tables():
    k = np.arange(SUB)[:, None]
    tables = []
    for first in range(RADIX):
        u = RADIX * np.arange(SUB)[None, :] + first
        angle = 2 * np.pi * (k * u % G) / G
        high, low = np_split(np.concatenate([np.cos(angle), np.sin(angle)], 0))
        tables.append(np.concatenate([high, low], 1))
    return np.stack(tables)


def phases(cells, peers):
    columns = np.arange(G)[:, None]
    angle = 2 * np.pi * (columns * cells[None, :] % G) / G
    width = G // peers
    shape = (peers, width, len(cells))
    return np.cos(angle).reshape(shape), np.sin(angle).reshape(shape)


def column_tables(peers):
    cosine, sine = phases(V_LOW * np.arange(V_HIGH), peers)
    coarse = np.concatenate(
        [np.concatenate([cosine, sine], 2), np.concatenate([-sine, cosine], 2)], 1
    )
    high, low = np_split(coarse)
    coarse = np.concatenate([high, low, high], 2)
    cosine, sine = phases(np.arange(V_LOW), peers)
    high, low = np_split(np.concatenate([cosine, -sine], 1))
    fine = np.concatenate([high, low], 2)
    cosine, sine = phases(np.arange(KW), peers)
    taps = np.concatenate([cosine, -sine], 1).astype(np.float32)
    return coarse, fine, taps


def dot(a, b, transposed=False, **kw):
    dims = (((1,), (1,)), ((), ())) if transposed else (((1,), (0,)), ((), ()))
    return lax.dot_general(a, b, dims, preferred_element_type=F32, **kw)


def sort_kernel(live_ref, vis_ref, tile_ref, u_ref, v_ref, index_ref, out_ref, *, peers):
    channels, slots = vis_ref.shape[1:]
    lane = lax.broadcasted_iota(jnp.int32, (8, slots), 1)
    row = lax.broadcasted_iota(jnp.int32, (8, slots), 0)
    slot = lax.broadcasted_iota(jnp.int32, (slots, slots), 0)
    other = lax.broadcasted_iota(jnp.int32, (slots, slots), 1)
    earlier = jnp.where(slot < other, 1.0, 0.0).astype(BF16)
    for channel in range(channels):
        own = slice(channel, channel + 1)
        u_cell = jnp.minimum(tile_ref[own] * (G // peers) + u_ref[own], G - KW)
        tile = jnp.where(lane[:1] < live_ref[own], u_cell // SUB, TILES)
        member = jnp.where(row == tile, 1.0, 0.0)
        before = dot(member.astype(BF16), earlier)
        totals = jnp.sum(member, axis=1, keepdims=True)
        start = jnp.zeros((1, 1), F32)
        target = jnp.zeros((1, slots), F32)
        for t in range(TILES):
            target = jnp.where(tile == t, start + before[t : t + 1], target)
            start = start + totals[t : t + 1]
        target = jnp.where(tile == TILES, -1.0, target).astype(jnp.int32)
        moved = jnp.where(slot == target, 1.0, 0.0).astype(BF16)
        pieces = []
        for part in range(2):
            value = vis_ref[part, own]
            for _ in range(3):
                high = value.astype(BF16).astype(F32)
                pieces.append(high)
                value = value - high
        v_cell = v_ref[own]
        for cell in (u_cell, v_cell):
            pieces.append((cell // V_LOW).astype(F32))
            pieces.append((cell % V_LOW).astype(F32))
        pieces.append(index_ref[0, own].astype(F32))
        pieces.append(index_ref[1, own].astype(F32))
        pieces.append(jnp.zeros((16 - len(pieces), slots), F32))
        packed = dot(jnp.concatenate(pieces, axis=0).astype(BF16), moved, transposed=True)
        real = packed[0:1] + packed[1:2] + packed[2:3]
        imag = packed[3:4] + packed[4:5] + packed[5:6]
        out_ref[channel] = jnp.concatenate(
            [
                real,
                imag,
                packed[6:7] * V_LOW + packed[7:8],
                packed[8:9] * V_LOW + packed[9:10],
                packed[10:12],
                jnp.zeros((2, slots), F32),
            ],
            axis=0,
        )
        for t in range(TILES):
            out_ref[channel, 6:7, t * (slots // TILES) : t * (slots // TILES) + 1] = totals[t : t + 1]


def sorted_fields(peers, live_count, visibility, tile_of, u_within, v_cell, kernel_index):
    channels, slots = visibility.shape[1:]
    whole = pl.BlockSpec(memory_space=pltpu.VMEM)
    return pl.pallas_call(
        functools.partial(sort_kernel, peers=peers),
        in_specs=[whole] * 6,
        out_specs=whole,
        out_shape=jax.ShapeDtypeStruct((channels, 8, slots), F32),
        name="sort_by_tile",
    )(live_count, visibility, tile_of[:, :, 0], u_within, v_cell, kernel_index)


def image_kernel(
    base_ref, live_ref, kernel_ref, row_ref, coarse_ref, fine_ref, tap_ref, *refs,
    normalizer, peers,
):
    field_refs = refs[:peers]
    out_ref, packed_ref, spectrum_ref, kernel_halves_ref, grid_ref = refs[peers:]
    owners, share_rows, width = out_ref.shape
    me = base_ref[1]
    channel = pl.program_id(0)
    slots = field_refs[0].shape[2]
    table_rows = kernel_ref.shape[1]

    @pl.when(channel == 0)
    def _():
        high, low = split(
            dot(tap_ref[...], kernel_ref[...], precision=lax.Precision.HIGHEST)
        )
        spectrum_ref[...] = jnp.concatenate([high, low], axis=1)
        high = kernel_ref[...].astype(BF16).astype(F32)
        kernel_halves_ref[...] = jnp.concatenate([high, kernel_ref[...] - high], axis=0)

    lane = lax.broadcasted_iota(jnp.int32, (8, slots + LANES), 1)
    offsets = [jnp.int32(0)] * TILES
    packed_ref[...] = jnp.zeros_like(packed_ref)
    for peer in range(peers):
        fields = jnp.concatenate(
            [field_refs[peer][0], jnp.zeros((8, LANES), F32)], axis=1
        )
        first = jnp.int32(0)
        for tile in range(TILES):
            count = live_ref[peer, channel, tile]
            block = offsets[tile] // LANES
            within = offsets[tile] - block * LANES
            shift = within - first
            width_all = slots + LANES
            moved = pltpu.roll(fields, jnp.where(shift < 0, shift + width_all, shift), 1)
            kept = (lane >= within) & (lane < within + count)
            window = pl.ds(pl.multiple_of(block * LANES, LANES), width_all)
            packed_ref[tile, :, window] = packed_ref[tile, :, window] + jnp.where(kept, moved, 0.0)
            first = first + count
            offsets[tile] = offsets[tile] + count

    grid_ref[...] = jnp.zeros_like(grid_ref)

    def add_chunk(tile, index, carry):
        fields = packed_ref[tile, :, pl.ds(pl.multiple_of(index * CHUNK, CHUNK), CHUNK)]
        real, imag = fields[0:1], fields[1:2]
        cells = fields[2:6].astype(jnp.int32)
        u_cell, v_cell, index_u, index_v = cells[0:1], cells[1:2], cells[2:3], cells[3:4]
        table_row = lax.broadcasted_iota(jnp.int32, (table_rows, CHUNK), 0)
        chosen_v = jnp.where(table_row == index_v, 1.0, 0.0).astype(BF16)
        footprint = dot(spectrum_ref[...], jnp.concatenate([chosen_v, chosen_v], axis=0))
        high_row = lax.broadcasted_iota(jnp.int32, (V_HIGH, CHUNK), 0)
        at_coarse = high_row == v_cell // V_LOW
        values = jnp.concatenate(
            [jnp.where(at_coarse, real, 0.0), jnp.where(at_coarse, imag, 0.0)], axis=0
        )
        high, low = split(values)
        coarse = dot(coarse_ref[...], jnp.concatenate([high, high, low], axis=0))
        low_row = lax.broadcasted_iota(jnp.int32, (V_LOW, CHUNK), 0)
        at_fine = jnp.where(low_row == v_cell % V_LOW, 1.0, 0.0).astype(BF16)
        fine = dot(fine_ref[...], jnp.concatenate([at_fine, at_fine], axis=0))
        a_re, a_im = coarse[:width], coarse[width:]
        b_re, b_im = fine[:width], fine[width:]
        c_re = a_re * b_re - a_im * b_im
        c_im = a_re * b_im + a_im * b_re
        d_re, d_im = footprint[:width], footprint[width:]
        column = jnp.concatenate(
            [c_re * d_re - c_im * d_im, c_re * d_im + c_im * d_re], axis=0
        )
        high, low = split(column)
        column = jnp.concatenate([high, low, high], axis=1)

        chosen_u = jnp.where(table_row == index_u, 1.0, 0.0).astype(BF16)
        taps = dot(kernel_halves_ref[...].astype(BF16), chosen_u)
        grid_row = lax.broadcasted_iota(jnp.int32, (WINDOW, CHUNK), 0)
        grid_row = grid_row + tile * (SUB // RADIX)
        rows = []
        for first in range(RADIX):
            tap = (first - u_cell) & (RADIX - 1)
            start = (u_cell + tap - first) // RADIX

            def tap_of(base):
                value = taps[base : base + 1]
                for t in range(1, RADIX):
                    value = jnp.where(tap == t, taps[base + t : base + t + 1], value)
                return value

            at_first = grid_row == start
            at_second = grid_row == start + 1
            halves = []
            for base in (0, KW):
                part = jnp.where(
                    at_first, tap_of(base), jnp.where(at_second, tap_of(base + RADIX), 0.0)
                )
                halves.append(part.astype(BF16))
            rows.append(jnp.concatenate([halves[0], halves[0], halves[1]], axis=1))
        tile_rows = dot(jnp.concatenate(rows, axis=0), column, transposed=True)
        for first in range(RADIX):
            start = first * BLOCK + tile * (SUB // RADIX)
            grid_ref[start : start + WINDOW, :] += tile_rows[first * WINDOW : (first + 1) * WINDOW]
        return carry

    for tile in range(TILES):
        chunks = (offsets[tile] + CHUNK - 1) // CHUNK
        lax.fori_loop(0, chunks, functools.partial(add_chunk, tile), 0)

    parts = []
    for first in range(RADIX):
        high, low = split(grid_ref[first * BLOCK : first * BLOCK + SUB, :])
        table = row_ref[first]
        table = jnp.concatenate([table[:, :SUB], table], axis=1)
        both = dot(table, jnp.concatenate([high, low, high], axis=0))
        re = both[:SUB, :width] + both[SUB:, width:]
        im = both[:SUB, width:] - both[SUB:, :width]
        parts.append((re, im))
    (r0, i0), (r1, i1), (r2, i2), (r3, i3) = parts
    ar, ai, br, bi = r0 + r2, i0 + i2, r0 - r2, i0 - i2
    cr, ci, dr, di = r1 + r3, i1 + i3, r1 - r3, i1 - i3
    images = [
        (ar + cr, ai + ci),
        (br + di, bi - dr),
        (ar - cr, ai - ci),
        (br - di, bi + dr),
    ]
    for block, (re, im) in enumerate(images):
        power = (re * re + im * im) * normalizer
        for row in range(0, SUB, share_rows):
            owner = (block * SUB + row) // share_rows
            turn = owner ^ me
            place = (turn & 1) * (owners // 2) + turn // 2
            part = power[row : row + share_rows]

            @pl.when(channel == 0)
            def _():
                out_ref[place] = part

            @pl.when(channel != 0)
            def _():
                out_ref[place] += part


def image_power(place, owners, live, gathered, kernel, normalizer):
    peers = len(gathered)
    channels, _, slots = gathered[0].shape
    width = G // peers
    coarse, fine, taps = column_tables(peers)
    table_rows = kernel.shape[0]
    whole = lambda shape: pl.BlockSpec(shape, lambda c, *_: (0,) * len(shape))
    own = lambda x: pl.BlockSpec((None,) + x.shape[1:], lambda c, b, *_: (b[0], 0, 0))
    rows = row_dft_tables()
    spec = pltpu.PrefetchScalarGridSpec(
        num_scalar_prefetch=2,
        grid=(channels,),
        in_specs=[
            whole((KW, table_rows)),
            whole(rows.shape),
            own(coarse),
            own(fine),
            own(taps),
        ]
        + [pl.BlockSpec((1, 8, slots), lambda c, *_: (c, 0, 0))] * peers,
        out_specs=whole((owners, G // owners, width)),
        scratch_shapes=[
            pltpu.VMEM((TILES, 8, peers * slots + LANES), F32),
            pltpu.VMEM((2 * width, 2 * table_rows), BF16),
            pltpu.VMEM((2 * KW, table_rows), F32),
            pltpu.VMEM((RADIX * BLOCK, 2 * width), F32),
        ],
    )
    return pl.pallas_call(
        functools.partial(image_kernel, normalizer=normalizer, peers=peers),
        grid_spec=spec,
        out_shape=jax.ShapeDtypeStruct((owners, G // owners, width), F32),
        compiler_params=pltpu.CompilerParams(dimension_semantics=("arbitrary",)),
        name="image_power",
    )(place, live, kernel.T, rows, coarse, fine, taps, *gathered)


def bin_kernel(freq_ref, bins_ref, *refs):
    share_ref, sums_ref, bins_t_ref = refs[-3:]
    share = refs[0][...]
    for ref in refs[1:-3]:
        share = share + ref[...]
    share_ref[...] = share
    bins_t_ref[...] = bins_ref[...].astype(F32).T
    rows, width = share.shape
    group = 8
    high_row = lax.broadcasted_iota(jnp.int32, (BIN_HIGH, width), 0)
    low_row = lax.broadcasted_iota(jnp.int32, (BIN_LOW, width), 0)

    def add_group(index, running):
        window = pl.ds(pl.multiple_of(index * group, group), group)
        bins = bins_t_ref[window, :].astype(jnp.int32)
        values = share_ref[window, :]
        high = values.astype(BF16).astype(F32)
        rest = values - high
        middle = rest.astype(BF16).astype(F32)
        low = rest - middle
        left, right = [], []
        for row in range(group):
            one = slice(row, row + 1)
            at_high = high_row == bins[one] // BIN_LOW
            at_low = low_row == bins[one] % BIN_LOW
            right.append(jnp.where(at_low, 1.0, 0.0).astype(BF16))
            pieces = [jnp.where(at_high, x[one], 0.0) for x in (high, middle, low)]
            pieces.append(jnp.where(at_high, 1.0, 0.0))
            left.append(jnp.concatenate(pieces, axis=0).astype(BF16))
        if width % LANES == 0:
            left, right = [jnp.concatenate(left, axis=1)], [jnp.concatenate(right, axis=1)]
        for a, b in zip(left, right):
            running = running + dot(a, b, transposed=True)
        return running

    zeros = jnp.zeros((4 * BIN_HIGH, BIN_LOW), F32)
    sums = lax.fori_loop(0, rows // group, add_group, zeros, unroll=4)
    pieces = [sums[i * BIN_HIGH : (i + 1) * BIN_HIGH] for i in range(4)]
    sums = jnp.concatenate([pieces[0] + pieces[1] + pieces[2], pieces[3]], axis=0)
    sums_ref[...] = jnp.broadcast_to(sums[None], sums_ref.shape)


def bin_power(freq_index, received, bin_map, devices):
    rows, width = received[0].shape
    if rows % LANES:
        bin_map = lax.dynamic_slice_in_dim(bin_map, freq_index[0] * rows, rows, 1)
        freq_index = jnp.zeros_like(freq_index)
    spec = pltpu.PrefetchScalarGridSpec(
        num_scalar_prefetch=1,
        grid=(1,),
        in_specs=[
            pl.BlockSpec((width, rows), lambda i, f: (0, f[0])),
        ]
        + [pl.BlockSpec((rows, width), lambda i, f: (0, 0))] * len(received),
        out_specs=[
            pl.BlockSpec((rows, width), lambda i, f: (0, 0)),
            pl.BlockSpec((devices, 2 * BIN_HIGH, BIN_LOW), lambda i, f: (0, 0, 0)),
        ],
        scratch_shapes=[pltpu.VMEM((rows, width), F32)],
    )
    return pl.pallas_call(
        bin_kernel,
        grid_spec=spec,
        out_shape=[
            jax.ShapeDtypeStruct((rows, width), F32),
            jax.ShapeDtypeStruct((devices, 2 * BIN_HIGH, BIN_LOW), F32),
        ],
        name="bin_power",
    )(freq_index, bin_map, *received)


def from_all(x, axis):
    peers = lax.axis_size(axis)
    turns = [[(i, (i + by) % peers) for i in range(peers)] for by in range(1, peers)]
    return [x] + [lax.ppermute(x, axis, pairs) for pairs in turns]


def shares_received(parts, axis):
    owners = lax.axis_size(axis)
    pairs = lambda turn: [(i, i ^ turn) for i in range(owners)]
    half = owners // 2
    other = lax.ppermute(parts[half:], axis, pairs(1))
    sums = [parts[p] + other[p] for p in range(half)]
    return [sums[0]] + [lax.ppermute(sums[p], axis, pairs(2 * p)) for p in range(1, half)]


def per_device(visibility, tile_of, u_within, v_cell, kernel_index, kernel, live_count, bin_map):
    base_count = lax.axis_size("base")
    freq_count = lax.axis_size("freq")
    channels_here, slots = visibility.shape[1:]
    fields = sorted_fields(
        base_count, live_count, visibility, tile_of, u_within, v_cell, kernel_index
    )
    gathered = from_all(fields, "base")
    step = slots // TILES
    live = jnp.stack([fields[:, 6, ::step] for fields in gathered]).astype(jnp.int32)
    normalizer = 1.0 / (channels_here * freq_count * slots * base_count)
    place = jnp.stack([lax.axis_index("base"), lax.axis_index("freq")])
    power_part = image_power(place, freq_count, live, gathered, kernel, normalizer)
    received = shares_received(power_part, "freq")
    power_share, sums = bin_power(
        lax.axis_index("freq")[None], received, bin_map, freq_count * base_count
    )
    sums = lax.all_to_all(sums, ("freq", "base"), split_axis=0, concat_axis=0)
    sums = jnp.sum(sums, axis=0)
    return power_share, (sums[:BIN_HIGH] / sums[BIN_HIGH:]).reshape(NBINS)


def solution(mesh):
    in_specs = (
        P(None, "freq", "base"),
        P("freq", "base", None),
        P("freq", "base"),
        P("freq", "base"),
        P(None, "freq", "base"),
        P(),
        P("freq", "base"),
        P("base", None),
    )
    out_specs = (P("freq", "base"), P())
    return jax.shard_map(
        per_device, mesh=mesh, in_specs=in_specs, out_specs=out_specs, check_vma=False
    )
```
